32 devices in a mesh: grp: 4 (over x, core), pw: 8 (over z, y).
Axes of the slice: x: 2, y: 2, z: 4, core: 2. Of those that a mesh axis runs over, the one named last changes fastest.
Arguments:
- row_orbitals: bfloat16 [16, 32768], P('grp', 'pw'), may hold values from -6 to 6
- orbitals: bfloat16 [512, 32768], P(None, 'pw'), may hold values from -6 to 6
- fitting: bfloat16 [32768, 1024], P('pw'), may hold values from -0.03125 to 0.03125
- partner_vertex: bfloat16 [16, 512, 1024], P('grp', 'pw'), may hold values from -6 to 6
- amplitudes: bfloat16 [256, 512, 512], P(None, 'pw'), may hold values from -0.00036621094 to 0.00036621094
Outputs:
- ladder: float32 [256, 16, 16], P('pw', 'grp')
The draws below stay inside these ranges and needn't reach their ends.
All inputs are finite; a program needn't handle non-finite values.
Results may differ from the reference program's by a relative error of at most 0.005.
Values may be sent and summed in bfloat16 or wider, within the bound.
No kernel may reach another device: no remote copies, remote signals or barrier semaphores. Data moves between devices by JAX's collectives and lax.ppermute only.
A program may use at most 128 MiB of HBM per device.

```python
import jax
import jax.numpy as jnp
from jax import lax

NV = 512
NAUX = 1024
GRID = 32768
ROWS = 16
PARTNERS = 16
NPAIR = 256


def levels(own_key, shape, split, smallest, high):
    factor_of, own = 1.0, jax.random.fold_in(own_key, 6)
    for dim, parts in split:
        steps = jnp.exp(jax.random.uniform(jax.random.fold_in(own, dim), (parts,), jnp.float32, smallest / len(split), high / len(split)))
        factor_of = factor_of * jnp.repeat(steps, shape[dim] // parts).reshape([-1 if axis == dim else 1 for axis in range(len(shape))])
    return factor_of


def noise(rng, extent, deviation, most, shards=(), kind=jnp.bfloat16):
    drawn = jax.random.normal(rng, extent, jnp.float32) * deviation
    if len(shards) > 0:
        drawn = levels(rng, extent, shards, -0.22, 0.18) * drawn
    return jnp.clip(drawn, min=-most, max=most).astype(kind)


def setup_inputs(seed: int = 0) -> dict:
    splits = jax.random.split(jax.random.key(seed), 6)
    return {
        "row_orbitals": noise(splits[0], (ROWS, GRID), 1.0, 6.0, ((0, 4), (1, 8))),
        "orbitals": noise(splits[1], (NV, GRID), 1.0, 6.0, ((1, 8),)),
        "fitting": noise(splits[2], (GRID, NAUX), GRID ** -0.5, 0.03125, ((0, 8),)),
        "partner_vertex": noise(splits[3], (PARTNERS, NV, NAUX), 1.0, 6.0, ((0, 4), (1, 8))),
        "amplitudes": noise(splits[4], (NPAIR, NV, NV), (NV * NV * NAUX) ** -0.5, 0.00036621094, ((1, 8),)),
    }


def reference(row_orbitals, orbitals, fitting, partner_vertex, amplitudes):
    orbit32 = orbitals.astype(jnp.float32)

    def one_row(row):
        pair = (row.astype(jnp.float32)[None, :] * orbit32).astype(jnp.bfloat16)
        return jnp.dot(pair, fitting, preferred_element_type=jnp.float32).astype(jnp.bfloat16)

    vertex = lax.map(one_row, row_orbitals)
    flat_partner = partner_vertex.reshape(PARTNERS * NV, NAUX)
    amp32 = amplitudes.astype(jnp.float32)

    def ladder_row(vrow):
        rungs = jnp.dot(vrow, flat_partner.T, preferred_element_type=jnp.float32).astype(jnp.bfloat16)
        rungs = rungs.reshape(NV, PARTNERS, NV).astype(jnp.float32)
        return jnp.einsum('cbd,icd->ib', rungs, amp32)

    result = lax.map(ladder_row, vertex)
    return jnp.transpose(result, (1, 0, 2))
```

```python
import jax
import jax.numpy as jnp
from jax import lax
from jax.experimental import pallas as pl
from jax.experimental.pallas import tpu as pltpu
from jax.sharding import PartitionSpec as P


NT = (((1,), (1,)), ((), ()))


def swap(value, axis, offset):
    if offset == 0:
        return value
    pairs = [(i, i ^ offset) for i in range(lax.axis_size(axis))]
    return lax.ppermute(value, axis, pairs)


def pair_kernel(where, row_ref, orb_ref, fit_ref, out_ref, wide):
    del where
    nrow, grid = row_ref.shape
    high = wide.shape[1]
    cloc = orb_ref.shape[2]

    @pl.when(pl.program_id(0) == 0)
    def _():
        for a in range(nrow):
            wide[a] = jnp.broadcast_to(row_ref[a : a + 1, :], (high, grid))

    block = orb_ref[0, 0].reshape(cloc // high, high, grid)
    pair = [(block * wide[a][None]).reshape(cloc, grid) for a in range(nrow)]
    part = jnp.dot(jnp.concatenate(pair, axis=0), fit_ref[...], preferred_element_type=jnp.float32)
    out_ref[...] = part.astype(out_ref.dtype).reshape(out_ref.shape)


def fitted(where, row, orbitals, fitting, naux, dtype):
    nrow, grid = row.shape
    nown, _, cloc, _ = orbitals.shape
    return pl.pallas_call(
        pair_kernel,
        grid_spec=pltpu.PrefetchScalarGridSpec(
            num_scalar_prefetch=1,
            grid=(nown,),
            in_specs=[
                pl.BlockSpec((nrow, grid), lambda s, w: (0, 0)),
                pl.BlockSpec((1, 1, cloc, grid), lambda s, w: (s, w[1], 0, 0)),
                pl.BlockSpec((grid, naux), lambda s, w: (0, w[0])),
            ],
            out_specs=pl.BlockSpec((nrow, 1, cloc, naux), lambda s, w: (0, s, 0, 0)),
            scratch_shapes=[pltpu.VMEM((nrow, 16, grid), jnp.bfloat16)],
        ),
        out_shape=jax.ShapeDtypeStruct((nrow, nown, cloc, naux), dtype),
        cost_estimate=pl.CostEstimate(
            flops=2 * nrow * nown * cloc * grid * naux, bytes_accessed=8 << 20, transcendentals=0
        ),
    )(where, row, orbitals, fitting)


def relay_kernel(amp_ref, out_ref):
    npair, high, _ = amp_ref.shape
    nz, _, _, wide = out_ref.shape
    lanes = wide // high
    n = high * high
    row = lax.broadcasted_iota(jnp.int32, (n, n), 0)
    col = lax.broadcasted_iota(jnp.int32, (n, n), 1)
    same = (row // high == col % high) & (row % high == col // high)
    turn = jnp.where(same, 1.0, 0.0).astype(jnp.bfloat16)
    for i in range(0, npair, high):
        block = amp_ref[i : i + high].reshape(n, nz * lanes)
        moved = jnp.dot(turn, block, preferred_element_type=jnp.float32).astype(jnp.bfloat16)
        for c in range(high):
            for z in range(nz):
                tile = moved[c * high : (c + 1) * high, z * lanes : (z + 1) * lanes]
                out_ref[z, 0, i : i + high, c * lanes : (c + 1) * lanes] = tile


def relay(amplitudes, lanes):
    npair, cloc, nvirt = amplitudes.shape
    high, nz = 16, 2
    shape = (nvirt // lanes, cloc // high, npair, high * lanes)
    return pl.pallas_call(
        relay_kernel,
        grid=(cloc // high, nvirt // lanes // nz),
        in_specs=[pl.BlockSpec((npair, high, nz * lanes), lambda c, d: (0, c, d))],
        out_specs=pl.BlockSpec((nz, 1, npair, high * lanes), lambda c, d: (d, c, 0, 0)),
        out_shape=jax.ShapeDtypeStruct(shape, jnp.bfloat16),
        cost_estimate=pl.CostEstimate(
            flops=2 * 256 * npair * cloc * nvirt, bytes_accessed=32 << 20, transcendentals=0
        ),
    )(amplitudes)


def ladder_kernel(where, v_ref, near_ref, far_ref, amp_ref, start_ref, out_ref, both, rungs):
    nb, width, naux = near_ref.shape

    @pl.when(pl.program_id(0) == 0)
    def _():
        out_ref[...] = start_ref[...]
        side = pl.multiple_of(where[1] * width, width)
        other = pl.multiple_of((1 - where[1]) * width, width)
        both[:, pl.ds(side, width), :] = near_ref[...]
        both[:, pl.ds(other, width), :] = far_ref[...]

    nc, na, _ = v_ref.shape
    lanes = 2 * width
    vertex = v_ref[...].reshape(nc * na, naux)
    for b in range(0, nb, 2):
        block = both[b : b + 2].reshape(2 * lanes, naux)
        part = lax.dot_general(vertex, block, NT, preferred_element_type=jnp.float32)
        part = part.astype(jnp.bfloat16)
        for i in range(2):
            for c in range(nc):
                tile = part[c * na : (c + 1) * na, i * lanes : (i + 1) * lanes]
                rungs[(b + i) * na : (b + i + 1) * na, c * lanes : (c + 1) * lanes] = tile
    out_ref[...] += lax.dot_general(
        rungs[...], amp_ref[0, 0], NT, preferred_element_type=jnp.float32
    )


def ladder_part(where, vertex, near, far, amps, start):
    cloc, na, naux = vertex.shape
    nb, width, _ = near.shape
    _, ncb, npair, wide = amps.shape
    step = cloc // ncb
    rows = nb * na
    return pl.pallas_call(
        ladder_kernel,
        grid_spec=pltpu.PrefetchScalarGridSpec(
            num_scalar_prefetch=1,
            grid=(ncb,),
            in_specs=[
                pl.BlockSpec((step, na, naux), lambda s, w: (s, 0, 0)),
                pl.BlockSpec((nb, width, naux), lambda s, w: (0, 0, 0)),
                pl.BlockSpec((nb, width, naux), lambda s, w: (0, 0, 0)),
                pl.BlockSpec((1, 1, npair, wide), lambda s, w: (w[0], s, 0, 0)),
                pl.BlockSpec((rows, npair), lambda s, w: (0, 0)),
            ],
            out_specs=pl.BlockSpec((rows, npair), lambda s, w: (0, 0)),
            scratch_shapes=[
                pltpu.VMEM((nb, 2 * width, naux), jnp.bfloat16),
                pltpu.VMEM((rows, wide), jnp.bfloat16),
            ],
        ),
        out_shape=jax.ShapeDtypeStruct((rows, npair), jnp.float32),
        cost_estimate=pl.CostEstimate(
            flops=2 * cloc * na * nb * 2 * width * (naux + npair),
            bytes_accessed=8 << 20,
            transcendentals=0,
        ),
    )(where, vertex, near, far, amps, start)


def local(row_orbitals, orbitals, fitting, partner_vertex, amplitudes):
    ngrp, npw = lax.axis_size("grp"), lax.axis_size("pw")
    g, w = lax.axis_index("grp"), lax.axis_index("pw")
    bits = npw.bit_length() - 1
    nrow, grid = row_orbitals.shape
    nvirt, naux = orbitals.shape[0], fitting.shape[1]
    cloc, aux = nvirt // npw, naux // ngrp
    npair = amplitudes.shape[0]
    nb = partner_vertex.shape[0]

    rows = [swap(row_orbitals, "grp", k) for k in range(ngrp)]

    pieces = []
    for k in range(ngrp):
        cut = lax.dynamic_slice_in_dim(partner_vertex, (g ^ k) * aux, aux, axis=2)
        pieces.append(swap(cut, "grp", k))
    blocks = {0: jnp.concatenate(pieces, axis=0)}
    for bit in reversed(range(1, bits)):
        for o in list(blocks):
            blocks[o ^ (1 << bit)] = swap(blocks[o], "pw", 1 << bit)

    split = orbitals.reshape(npw // 2, 2, cloc, grid)
    mine = jnp.stack([g, w & 1]).astype(jnp.int32)
    theirs = jnp.stack([g, 1 - (w & 1)]).astype(jnp.int32)
    sent = [swap(fitted(theirs, row, split, fitting, aux, jnp.bfloat16), "pw", 1) for row in rows]
    chunks = []
    for k in range(ngrp):
        total = fitted(mine, rows[k], split, fitting, aux, jnp.float32) + sent[k].astype(jnp.float32)
        for bit in range(1, bits):
            halves = total.reshape(nrow, total.shape[1] // 2, 2, cloc, aux)
            side = (w >> bit) & 1
            keep = lax.dynamic_index_in_dim(halves, side, 2, keepdims=False)
            give = lax.dynamic_index_in_dim(halves, 1 - side, 2, keepdims=False)
            got = swap(give.astype(jnp.bfloat16), "pw", 1 << bit)
            total = keep + got.astype(jnp.float32)
        chunks.append(total[:, 0].astype(jnp.bfloat16))
    vertex = jnp.concatenate(chunks, axis=0).transpose(1, 0, 2)

    for o in list(blocks):
        blocks[o ^ 1] = swap(blocks[o], "pw", 1)

    rows_out = ngrp * nb * ngrp * nrow
    pairw = 2 * cloc
    nvert = npw // 2
    if pairw % 128 == 0 and cloc % 16 == 0:
        amps = relay(amplitudes, pairw)
        total = jnp.zeros((rows_out, npair), jnp.float32)
        for o in sorted(o for o in blocks if not o & 1):
            where = jnp.stack([(w ^ o) >> 1, w & 1]).astype(jnp.int32)
            total = ladder_part(where, vertex, blocks[o], blocks[o ^ 1], amps, total)
    else:
        total = jnp.zeros((ngrp * nb, ngrp * nrow, npair), jnp.float32)
        for o, block in blocks.items():
            amp = lax.dynamic_slice_in_dim(amplitudes, (w ^ o) * cloc, cloc, axis=2)
            rungs = jnp.einsum("cap,bdp->cabd", vertex, block, preferred_element_type=jnp.float32)
            rungs = rungs.astype(jnp.bfloat16)
            total += jnp.einsum("cabd,icd->bai", rungs, amp, preferred_element_type=jnp.float32)

    total = total.reshape(ngrp, nb, ngrp, nrow, npair)
    gbits = ngrp.bit_length() - 1
    summed = 0.0
    for k in range(ngrp):
        got = swap(total[:, :, k], "grp", k).reshape((2,) * gbits + (nb, nrow, npair))
        summed += lax.rev(got, [gbits - 1 - j for j in range(gbits) if k >> j & 1])
    parts = summed.reshape(ngrp * nb * nrow, npw, npair // npw)
    result = 0.0
    for o in range(npw):
        cut = lax.dynamic_index_in_dim(parts, w ^ o, 1, keepdims=False)
        result += swap(cut, "pw", o)
    result = result.reshape((2,) * gbits + (nb, nrow, npair // npw))
    for j in range(gbits):
        result = jnp.where((g >> j) & 1, lax.rev(result, [gbits - 1 - j]), result)
    result = result.reshape(ngrp * nb, nrow, npair // npw)
    return result.transpose(2, 1, 0)


def solution(mesh):
    placed = (
        P("grp", "pw"),
        P(None, "pw"),
        P("pw", None),
        P("grp", "pw", None),
        P(None, "pw", None),
    )
    return jax.shard_map(
        local, mesh=mesh, in_specs=placed, out_specs=P("pw", "grp", None), check_vma=False
    )
```
